32 devices in a mesh: row: 16 (over z, y, core), col: 2 (over x).
Axes of the slice: x: 2, y: 2, z: 4, core: 2. Of those that a mesh axis runs over, the one named last changes fastest.
Arguments:
- diag_tile: float32 [1024, 1024], P(('row', 'col')), as said below
- left_row: bfloat16 [1024, 32, 256], P('col', 'row'), may hold values from -0.3984375 to 0.3984375
- right_row: bfloat16 [1024, 32, 256], P('col', 'row'), may hold values from -1.09375 to 1.09375
- right_col: bfloat16 [1024, 8, 256], P('row', 'col'), may hold values from -1.09375 to 1.09375
- bucket_row: int32 [32], P('row'), may hold values from 1 to 4
- bucket_col: int32 [8], P('col'), may hold values from 1 to 4
Outputs:
- panel_row: bfloat16 [1024, 32, 256], P('col', 'row')
- panel_col: bfloat16 [1024, 8, 256], P('row', 'col')
- update_left: bfloat16 [32, 8, 1024, 256], P('row', 'col')
The draws below stay inside these ranges and needn't reach their ends.
Inputs may be any that keep to these rules, and one draw needn't show every extreme that they name: diag_tile is symmetric positive definite. `bucket_row`: a tile's rank is 64 times its bucket; factor columns from the rank on are not part of the tile. `bucket_col`: as for bucket_row.
All inputs are finite; a program needn't handle non-finite values.
Results may differ from the reference program's by a relative error of at most 0.0062.
Values may be sent and summed in bfloat16 or wider, within the bound.
A program may use at most 128 MiB of HBM per device.

```python
import jax
import jax.numpy as jnp
from jax import lax

NB = 1024
RMAX = 256
RSTEP = 64
MT = 32
NC = 8


def draw_diag_tile(key, part):
    first = jax.random.fold_in(jax.random.fold_in(key, 11), 0)
    factor = jax.random.normal(first, (NB, NB), jnp.float32) / jnp.sqrt(jnp.float32(NB))
    gram = jnp.dot(factor, factor.T, precision=lax.Precision.HIGHEST) + jnp.eye(NB, dtype=jnp.float32)
    return 0.5 * (gram + gram.T)


def with_ends(drawn, key, least, high):
    spot = [jax.random.randint(jax.random.fold_in(key, axis), (), 0, length) for axis, length in enumerate(drawn.shape)]
    main_axis = drawn.shape.index(max(drawn.shape))
    next_to = spot[:main_axis] + [(spot[main_axis] + 1) % drawn.shape[main_axis]] + spot[main_axis + 1:]
    return drawn.at[tuple(spot)].set(least).at[tuple(next_to)].set(high)


def level_of(rng, extent, cuts, smallest, high):
    factor_of = 1.0
    for axis_at, parts in cuts:
        draws = jax.random.uniform(jax.random.fold_in(jax.random.fold_in(rng, 6), axis_at), (parts,), jnp.float32, smallest / len(cuts), high / len(cuts))
        factor_of = factor_of * jnp.repeat(jnp.exp(draws), extent[axis_at] // parts).reshape((-1,) + (1,) * (len(extent) - 1 - axis_at))
    return factor_of


def normal_values(stream_key, extent, scale, limit, shards=(), kind=jnp.bfloat16):
    factor_of = level_of(stream_key, extent, shards, -0.22, 0.18) if shards else 1.0
    result = jax.random.normal(stream_key, extent, jnp.float32) * scale * factor_of
    return jnp.minimum(jnp.maximum(result, -limit), limit).astype(kind)


def setup_inputs(seed: int = 0) -> dict:
    splits = jax.random.split(jax.random.key(seed), 7)
    diag_tile = draw_diag_tile(jax.random.fold_in(splits[6], 71), 0)
    left_row = normal_values(splits[1], (NB, MT, RMAX), 0.0625, 0.3984375, ((0, 2), (1, 16)))
    right_row = normal_values(splits[2], (NB, MT, RMAX), 0.18, 1.09375, ((0, 2), (1, 16)))
    right_col = normal_values(splits[3], (NB, NC, RMAX), 0.18, 1.09375, ((0, 16), (1, 2)))
    bucket_row = with_ends(jax.random.randint(splits[4], (MT,), 1, 5), jax.random.fold_in(splits[4], 1), 1, 4).astype(jnp.int32)
    bucket_col = with_ends(jax.random.randint(splits[5], (NC,), 1, 5), jax.random.fold_in(splits[5], 1), 1, 4).astype(jnp.int32)
    return dict(diag_tile=diag_tile, left_row=left_row, right_row=right_row, right_col=right_col, bucket_row=bucket_row, bucket_col=bucket_col)


def solve_panel(inverse, right, bucket):
    live = jnp.arange(RMAX, dtype=jnp.int32)[None, :] < (RSTEP * bucket)[:, None]
    masked = jnp.where(live[None, :, :], right, jnp.zeros_like(right))
    flat = masked.astype(jnp.float32).reshape(NB, -1)
    solved = jnp.dot(inverse.astype(jnp.float32), flat.astype(jnp.float32), precision=lax.Precision.HIGHEST, preferred_element_type=jnp.float32)
    return solved.reshape(NB, bucket.shape[0], RMAX).astype(jnp.bfloat16)

def reference(diag_tile, left_row, right_row, right_col, bucket_row, bucket_col):
    lower_factor = jnp.linalg.cholesky(diag_tile)
    identity = jnp.eye(NB, dtype=jnp.float32)
    inverse = lax.linalg.triangular_solve(lower_factor, identity, left_side=True, lower=True)
    panel_row = solve_panel(inverse, right_row, bucket_row)
    panel_col = solve_panel(inverse, right_col, bucket_col)
    col_wide = panel_col.astype(jnp.float32)

    def one_tile(operands):
        basis, factor = operands
        coupling = jnp.einsum('ka,kjb->jab', factor.astype(jnp.float32), col_wide, precision=lax.Precision.HIGHEST).astype(jnp.bfloat16)
        update = jnp.einsum('ka,jab->jkb', basis.astype(jnp.float32), coupling.astype(jnp.float32), precision=lax.Precision.HIGHEST)
        return (-update).astype(jnp.bfloat16)
    update_left = lax.map(one_tile, (jnp.moveaxis(left_row, 1, 0), jnp.moveaxis(panel_row, 1, 0)))
    return (panel_row, panel_col, update_left)
```

```python
import functools

import jax
import jax.numpy as jnp
from jax import lax
from jax.experimental import pallas as pl
from jax.experimental.pallas import tpu as pltpu
from jax.sharding import PartitionSpec as P

RSTEP = 64
BLOCK = 128
SUB = 8
HI = lax.Precision.HIGHEST


def dot_nn(a, b):
    return lax.dot_general(a, b, (((1,), (0,)), ((), ())), precision=HI, preferred_element_type=jnp.float32)


def dot_nt(a, b):
    return lax.dot_general(a, b, (((1,), (1,)), ((), ())), precision=HI, preferred_element_type=jnp.float32)


def factor_block(d_ref, t_ref):
    size = d_ref.shape[0]
    steps = size // SUB
    shape = (SUB, size)
    lane = lax.broadcasted_iota(jnp.int32, shape, 1)
    sub = lax.broadcasted_iota(jnp.int32, shape, 0)
    rows = [d_ref[SUB * i : SUB * (i + 1), :] for i in range(steps)]
    for p in range(steps):
        base = SUB * p
        pivot = (lane >= base) & (lane < base + SUB)
        top = rows[p]
        cols = [jnp.broadcast_to(top[:, base + s : base + s + 1], shape) for s in range(SUB)]
        e = [[jnp.broadcast_to(cols[s][i : i + 1, :], shape) if s <= i else None for s in range(SUB)] for i in range(SUB)]
        top = jnp.where(pivot, jnp.where(lane - base == sub, 1.0, 0.0), top)
        u = [jnp.broadcast_to(top[s : s + 1, :], shape) for s in range(SUB)]
        inv = [None] * SUB
        for s in range(SUB):
            inv[s] = lax.rsqrt(e[s][s])
            u[s] = u[s] * inv[s]
            for i in range(s + 1, SUB):
                e[i][s] = e[i][s] * inv[s]
            for q in range(s + 1, SUB):
                for i in range(q, SUB):
                    e[i][q] = e[i][q] - e[i][s] * e[q][s]
                u[q] = u[q] - e[q][s] * u[s]
        out = u[0]
        for s in range(1, SUB):
            out = jnp.where(sub == s, u[s], out)
        t_ref[base : base + SUB, :] = jnp.where(lane <= base + sub, out, 0.0)
        z = list(u)
        for s in reversed(range(SUB)):
            z[s] = z[s] * inv[s]
            for q in range(s):
                z[q] = z[q] - e[s][q] * z[s]
        for i in range(p + 1, steps):
            m = rows[i]
            acc = jnp.where(pivot, 0.0, m)
            for s in range(SUB):
                acc = acc - jnp.broadcast_to(m[:, base + s : base + s + 1], shape) * z[s]
            rows[i] = acc


def inverse_kernel(a_ref, xh_ref, xl_ref, low, inv, work, block, tri):
    order = a_ref.shape[0]
    count = order // BLOCK

    def store(r, c0, c1, value):
        hi = value.astype(jnp.bfloat16)
        xh_ref[r : r + BLOCK, c0:c1] = hi
        xl_ref[r : r + BLOCK, c0:c1] = (value - hi.astype(jnp.float32)).astype(jnp.bfloat16)

    def step(j, carry):
        for jj in range(count):
            at = BLOCK * jj

            @pl.when(j == jj)
            def _():
                if jj == 0:
                    work[...] = a_ref[:, :BLOCK]
                    block[...] = a_ref[:BLOCK, :BLOCK]
                else:
                    got = a_ref[at:, at : at + BLOCK] - dot_nt(low[at:, :at], low[at : at + BLOCK, :at])
                    work[at:, :] = got
                    block[...] = got[:BLOCK, :]

        factor_block(block, tri)
        for jj in range(count):
            at = BLOCK * jj

            @pl.when(j == jj)
            def _():
                t = tri[...]
                if jj + 1 < count:
                    low[at + BLOCK :, at : at + BLOCK] = dot_nt(work[at + BLOCK :, :], t)
                if jj:
                    x = -dot_nn(t, dot_nn(low[at : at + BLOCK, :at], inv[:at, :at]))
                    inv[at : at + BLOCK, :at] = x
                    store(at, 0, at, x)
                inv[at : at + BLOCK, at : at + BLOCK] = t
                store(at, at, at + BLOCK, t)
                if jj + 1 < count:
                    inv[at : at + BLOCK, at + BLOCK :] = jnp.zeros((BLOCK, order - at - BLOCK), jnp.float32)
                    xh_ref[at : at + BLOCK, at + BLOCK :] = jnp.zeros((BLOCK, order - at - BLOCK), jnp.bfloat16)
                    xl_ref[at : at + BLOCK, at + BLOCK :] = jnp.zeros((BLOCK, order - at - BLOCK), jnp.bfloat16)

        return carry

    lax.fori_loop(0, count, step, 0)


def inverse_of(tile):
    order = tile.shape[0]
    return pl.pallas_call(
        inverse_kernel,
        out_shape=[jax.ShapeDtypeStruct((order, order), jnp.bfloat16)] * 2,
        in_specs=[pl.BlockSpec(memory_space=pltpu.VMEM)],
        out_specs=[pl.BlockSpec(memory_space=pltpu.VMEM)] * 2,
        scratch_shapes=[
            pltpu.VMEM((order, order), jnp.float32),
            pltpu.VMEM((order, order), jnp.float32),
            pltpu.VMEM((order, BLOCK), jnp.float32),
            pltpu.VMEM((BLOCK, BLOCK), jnp.float32),
            pltpu.VMEM((BLOCK, BLOCK), jnp.float32),
        ],
        compiler_params=pltpu.CompilerParams(vmem_limit_bytes=40 * 2**20),
        cost_estimate=pl.CostEstimate(flops=60 * 10**9, bytes_accessed=8 * order * order, transcendentals=0),
    )(tile)


def mask_columns(right, bucket):
    live = jnp.arange(right.shape[2], dtype=jnp.int32)[None, :] < (RSTEP * bucket)[:, None]
    return jnp.where(live[None, :, :], right, jnp.zeros_like(right))


def solve_whole(high, low, gathered):
    flat = gathered.reshape(gathered.shape[0], -1)
    solved = jnp.dot(high, flat, preferred_element_type=jnp.float32) + jnp.dot(
        low, flat, preferred_element_type=jnp.float32
    )
    return solved.astype(jnp.bfloat16).reshape(gathered.shape)


def per_device(diag_tile, left_row, right_row, right_col, bucket_row, bucket_col):
    whole_tile = lax.all_gather(diag_tile, ("row", "col"), axis=0, tiled=True)
    high, low = inverse_of(whole_tile)
    masked_row = mask_columns(right_row, bucket_row)
    masked_col = mask_columns(right_col, bucket_col)
    row_position = lax.axis_index("col")
    col_position = lax.axis_index("row")
    full_row = solve_whole(high, low, lax.all_gather(masked_row, "col", axis=0, tiled=True))
    full_col = solve_whole(high, low, lax.all_gather(masked_col, "row", axis=0, tiled=True))
    panel_row = lax.dynamic_slice_in_dim(
        full_row, row_position * masked_row.shape[0], masked_row.shape[0], 0
    )
    panel_col = lax.dynamic_slice_in_dim(
        full_col, col_position * masked_col.shape[0], masked_col.shape[0], 0
    )
    coupling = jnp.einsum(
        "kia,kjb->ijab", full_row, full_col, preferred_element_type=jnp.float32
    ).astype(jnp.bfloat16)
    update = jnp.einsum(
        "kia,ijab->ijkb",
        lax.all_gather(left_row, "col", axis=0, tiled=True),
        coupling,
        preferred_element_type=jnp.float32,
    )
    update_left = (-update).astype(jnp.bfloat16)
    return (panel_row, panel_col, update_left)


def solution(mesh):
    return jax.shard_map(
        per_device,
        mesh=mesh,
        in_specs=(
            P(("row", "col"), None),
            P("col", "row", None),
            P("col", "row", None),
            P("row", "col", None),
            P("row"),
            P("col"),
        ),
        out_specs=(P("col", "row", None), P("row", "col", None), P("row", "col", None, None)),
        check_vma=False,
    )
```

```python
import functools

import jax
import jax.numpy as jnp
from jax import lax
from jax.experimental import pallas as pl
from jax.experimental.pallas import tpu as pltpu
from jax.sharding import PartitionSpec as P

RSTEP = 64
BLOCK = 128
SUB = 8
HI = lax.Precision.HIGHEST


def dot_nn(a, b):
    return lax.dot_general(a, b, (((1,), (0,)), ((), ())), precision=HI, preferred_element_type=jnp.float32)


def dot_nt(a, b):
    return lax.dot_general(a, b, (((1,), (1,)), ((), ())), precision=HI, preferred_element_type=jnp.float32)


def factor_block(d_ref, t_ref):
    size = d_ref.shape[0]
    steps = size // SUB
    shape = (SUB, size)
    lane = lax.broadcasted_iota(jnp.int32, shape, 1)
    sub = lax.broadcasted_iota(jnp.int32, shape, 0)
    rows = [d_ref[SUB * i : SUB * (i + 1), :] for i in range(steps)]
    for p in range(steps):
        base = SUB * p
        pivot = (lane >= base) & (lane < base + SUB)
        top = rows[p]
        cols = [jnp.broadcast_to(top[:, base + s : base + s + 1], shape) for s in range(SUB)]
        e = [[jnp.broadcast_to(cols[s][i : i + 1, :], shape) if s <= i else None for s in range(SUB)] for i in range(SUB)]
        top = jnp.where(pivot, jnp.where(lane - base == sub, 1.0, 0.0), top)
        u = [jnp.broadcast_to(top[s : s + 1, :], shape) for s in range(SUB)]
        inv = [None] * SUB
        for s in range(SUB):
            inv[s] = lax.rsqrt(e[s][s])
            u[s] = u[s] * inv[s]
            for i in range(s + 1, SUB):
                e[i][s] = e[i][s] * inv[s]
            for q in range(s + 1, SUB):
                for i in range(q, SUB):
                    e[i][q] = e[i][q] - e[i][s] * e[q][s]
                u[q] = u[q] - e[q][s] * u[s]
        out = u[0]
        for s in range(1, SUB):
            out = jnp.where(sub == s, u[s], out)
        t_ref[base : base + SUB, :] = jnp.where(lane <= base + sub, out, 0.0)
        z = list(u)
        for s in reversed(range(SUB)):
            z[s] = z[s] * inv[s]
            for q in range(s):
                z[q] = z[q] - e[s][q] * z[s]
        for i in range(p + 1, steps):
            m = rows[i]
            acc = jnp.where(pivot, 0.0, m)
            for s in range(SUB):
                acc = acc - jnp.broadcast_to(m[:, base + s : base + s + 1], shape) * z[s]
            rows[i] = acc


def inverse_kernel(a_ref, xh_ref, xl_ref, low, inv, work, block, tri):
    order = a_ref.shape[0]
    count = order // BLOCK

    def store(r, c0, c1, value):
        hi = value.astype(jnp.bfloat16)
        xh_ref[r : r + BLOCK, c0:c1] = hi
        xl_ref[r : r + BLOCK, c0:c1] = (value - hi.astype(jnp.float32)).astype(jnp.bfloat16)

    def step(j, carry):
        for jj in range(count):
            at = BLOCK * jj

            @pl.when(j == jj)
            def _():
                if jj == 0:
                    work[...] = a_ref[:, :BLOCK]
                    block[...] = a_ref[:BLOCK, :BLOCK]
                else:
                    got = a_ref[at:, at : at + BLOCK] - dot_nt(low[at:, :at], low[at : at + BLOCK, :at])
                    work[at:, :] = got
                    block[...] = got[:BLOCK, :]

        factor_block(block, tri)
        for jj in range(count):
            at = BLOCK * jj

            @pl.when(j == jj)
            def _():
                t = tri[...]
                if jj + 1 < count:
                    low[at + BLOCK :, at : at + BLOCK] = dot_nt(work[at + BLOCK :, :], t)
                if jj:
                    x = -dot_nn(t, dot_nn(low[at : at + BLOCK, :at], inv[:at, :at]))
                    inv[at : at + BLOCK, :at] = x
                    store(at, 0, at, x)
                inv[at : at + BLOCK, at : at + BLOCK] = t
                store(at, at, at + BLOCK, t)
                if jj + 1 < count:
                    inv[at : at + BLOCK, at + BLOCK :] = jnp.zeros((BLOCK, order - at - BLOCK), jnp.float32)
                    xh_ref[at : at + BLOCK, at + BLOCK :] = jnp.zeros((BLOCK, order - at - BLOCK), jnp.bfloat16)
                    xl_ref[at : at + BLOCK, at + BLOCK :] = jnp.zeros((BLOCK, order - at - BLOCK), jnp.bfloat16)

        return carry

    lax.fori_loop(0, count, step, 0)


def inverse_of(tile):
    order = tile.shape[0]
    return pl.pallas_call(
        inverse_kernel,
        out_shape=[jax.ShapeDtypeStruct((order, order), jnp.bfloat16)] * 2,
        in_specs=[pl.BlockSpec(memory_space=pltpu.VMEM)],
        out_specs=[pl.BlockSpec(memory_space=pltpu.VMEM)] * 2,
        scratch_shapes=[
            pltpu.VMEM((order, order), jnp.float32),
            pltpu.VMEM((order, order), jnp.float32),
            pltpu.VMEM((order, BLOCK), jnp.float32),
            pltpu.VMEM((BLOCK, BLOCK), jnp.float32),
            pltpu.VMEM((BLOCK, BLOCK), jnp.float32),
        ],
        compiler_params=pltpu.CompilerParams(vmem_limit_bytes=40 * 2**20),
        cost_estimate=pl.CostEstimate(flops=60 * 10**9, bytes_accessed=8 * order * order, transcendentals=0),
    )(tile)


def gather_kernel(rows, cols, groups, x_ref, out_ref, send_sem, recv_sem):
    order = out_ref.shape[2]
    pairs = rows // groups // 2
    row = lax.axis_index("row")
    col = lax.axis_index("col")
    group = row // (2 * pairs)
    pair = (row // 2) % pairs
    core = row % 2
    offsets = [(a, b) for a in range(pairs) for b in range(cols)]

    def device(g, p, c):
        return {"row": (g * pairs + p) * 2 + core, "col": c}

    def block(g, p, c, k):
        return ((g * pairs + p) * 2 + k) * cols + c

    def width(g):
        return -(-order * (g + 1) // (groups * BLOCK)) * BLOCK

    def copy(source, index, wide, sem, target):
        return pltpu.make_async_remote_copy(
            src_ref=source.at[:, :wide],
            dst_ref=out_ref.at[index, :, :wide],
            send_sem=send_sem.at[sem],
            recv_sem=recv_sem.at[index],
            device_id=target,
            device_id_type=pl.DeviceIdType.MESH,
        )

    partner = {"row": (group * pairs + pair) * 2 + 1 - core, "col": col}
    ring = [device((group + k) % groups, pair, col) for k in range(1, groups)]
    plane = [device(group, (pair + a) % pairs, (col + b) % cols) for a, b in offsets[1:]]
    barrier = pltpu.get_barrier_semaphore()
    for peer in ring + plane + [partner]:
        pl.semaphore_signal(barrier, inc=1, device_id=peer, device_id_type=pl.DeviceIdType.MESH)
    pl.semaphore_wait(barrier, len(ring) + len(plane) + 1)

    own = block(group, pair, col, core)
    for g in range(groups):

        @pl.when(group == g)
        def _():
            for k, peer in enumerate(ring):
                copy(x_ref, own, width(g), k, peer).start()
            for k, peer in enumerate(plane):
                copy(x_ref, own, width(g), groups + g * len(offsets) + k, peer).start()
            copy(x_ref, own, width(g), groups * (1 + len(offsets)) + g * len(offsets), partner).start()

    out_ref[own] = x_ref[...]
    for g in range(groups):

        @pl.when(group != g)
        def _():
            index = block(g, pair, col, core)
            got = out_ref.at[index]
            copy(got, index, width(g), 0, partner).wait_recv()
            for k, peer in enumerate(plane):
                copy(got, index, width(g), groups + g * len(offsets) + k, peer).start()
            copy(got, index, width(g), groups * (1 + len(offsets)) + g * len(offsets), partner).start()

    for g in range(groups):
        for n, (a, b) in enumerate(offsets):
            if n:
                index = block(g, (pair + a) % pairs, (col + b) % cols, core)
                got = out_ref.at[index]
                copy(got, index, width(g), 0, partner).wait_recv()
                copy(got, index, width(g), groups * (1 + len(offsets)) + g * len(offsets) + n, partner).start()

    for g in range(groups):
        for n, (a, b) in enumerate(offsets):
            index = block(g, (pair + a) % pairs, (col + b) % cols, 1 - core)
            copy(out_ref.at[index], index, width(g), 0, partner).wait_recv()

    for g in range(groups):

        @pl.when(group == g)
        def _():
            for k, peer in enumerate(ring):
                copy(x_ref, own, width(g), k, peer).wait_send()

        for k, peer in enumerate(plane):
            copy(x_ref, own, width(g), groups + g * len(offsets) + k, peer).wait_send()
        for n in range(len(offsets)):
            copy(x_ref, own, width(g), groups * (1 + len(offsets)) + g * len(offsets) + n, partner).wait_send()


def gather_tile(part, rows, cols):
    high, order = part.shape
    groups = 4 if rows % 8 == 0 else 1
    sends = groups * (1 + 2 * (rows // groups // 2) * cols)
    blocks = pl.pallas_call(
        functools.partial(gather_kernel, rows, cols, groups),
        out_shape=jax.ShapeDtypeStruct((rows * cols, high, order), part.dtype),
        in_specs=[pl.BlockSpec(memory_space=pltpu.VMEM)],
        out_specs=pl.BlockSpec(memory_space=pltpu.VMEM),
        scratch_shapes=[pltpu.SemaphoreType.DMA((sends,)), pltpu.SemaphoreType.DMA((rows * cols,))],
        compiler_params=pltpu.CompilerParams(collective_id=0, has_side_effects=True),
        cost_estimate=pl.CostEstimate(flops=20 * 10**9, bytes_accessed=4 * order * order, transcendentals=0),
    )(part)
    return blocks.reshape(order, order)


def tail_kernel(xh_ref, xl_ref, v_ref, w_ref, u_ref, row_ref, col_ref, out_ref, coupling):
    order = xh_ref.shape[0]
    tiles = out_ref.shape[1]
    rank = v_ref.shape[1]
    chunk = 256

    def solve(src, dst):
        for at in range(0, order, chunk):
            end = at + chunk
            got = jnp.dot(xh_ref[at:end, :end], src[:end, :], preferred_element_type=jnp.float32)
            got = got + jnp.dot(xl_ref[at:end, :end], src[:end, :], preferred_element_type=jnp.float32)
            dst[at:end, :] = got.astype(jnp.bfloat16)

    @pl.when(pl.program_id(0) == 0)
    def _():
        for j in range(tiles):
            solve(w_ref.at[:, rank * j : rank * (j + 1)], col_ref.at[:, rank * j : rank * (j + 1)])

    solve(v_ref, row_ref)
    coupling[...] = lax.dot_general(
        row_ref[...], col_ref[...], (((0,), (0,)), ((), ())), preferred_element_type=jnp.float32
    ).astype(jnp.bfloat16)
    for j in range(tiles):
        for at in range(0, order, chunk):
            got = jnp.dot(
                u_ref[at : at + chunk, :], coupling[:, rank * j : rank * (j + 1)], preferred_element_type=jnp.float32
            )
            out_ref[0, j, at : at + chunk, :] = (-got).astype(jnp.bfloat16)


def tail(high, low, v, w, u, rank):
    order = high.shape[0]
    count, tiles = v.shape[1] // rank, w.shape[1] // rank
    whole = pl.BlockSpec((order, order), lambda i: (0, 0))
    wide = pl.BlockSpec(w.shape, lambda i: (0, 0))
    one = pl.BlockSpec((order, rank), lambda i: (0, i))
    return pl.pallas_call(
        tail_kernel,
        grid=(count,),
        out_shape=[
            jax.ShapeDtypeStruct(v.shape, jnp.bfloat16),
            jax.ShapeDtypeStruct(w.shape, jnp.bfloat16),
            jax.ShapeDtypeStruct((count, tiles, order, rank), jnp.bfloat16),
        ],
        in_specs=[whole, whole, one, wide, one],
        out_specs=[one, wide, pl.BlockSpec((1, tiles, order, rank), lambda i: (i, 0, 0, 0))],
        scratch_shapes=[pltpu.VMEM((rank, w.shape[1]), jnp.bfloat16)],
        compiler_params=pltpu.CompilerParams(vmem_limit_bytes=50 * 2**20),
        cost_estimate=pl.CostEstimate(flops=8 * 10**9, bytes_accessed=18 * order * order, transcendentals=0),
    )(high, low, v, w, u)


def mask_columns(right, bucket):
    live = jnp.arange(right.shape[2], dtype=jnp.int32)[None, :] < (RSTEP * bucket)[:, None]
    return jnp.where(live[None, :, :], right, jnp.zeros_like(right))


def per_device(rows, cols, diag_tile, left_row, right_row, right_col, bucket_row, bucket_col):
    rank = right_row.shape[2]
    flat_row = mask_columns(right_row, bucket_row).reshape(right_row.shape[0], -1)
    flat_col = mask_columns(right_col, bucket_col).reshape(right_col.shape[0], -1)
    flat_left = left_row.reshape(left_row.shape[0], -1)
    v = lax.all_gather(flat_row, "col", axis=0, tiled=True)
    w = lax.all_gather(flat_col, "row", axis=0, tiled=True)
    u = lax.all_gather(flat_left, "col", axis=0, tiled=True)
    high, low = inverse_of(gather_tile(diag_tile, rows, cols))
    full_row, full_col, update_left = tail(high, low, v, w, u, rank)
    panel_row = lax.dynamic_slice_in_dim(
        full_row, lax.axis_index("col") * flat_row.shape[0], flat_row.shape[0], 0
    ).reshape(right_row.shape)
    panel_col = lax.dynamic_slice_in_dim(
        full_col, lax.axis_index("row") * flat_col.shape[0], flat_col.shape[0], 0
    ).reshape(right_col.shape)
    return (panel_row, panel_col, update_left)


def solution(mesh):
    return jax.shard_map(
        functools.partial(per_device, mesh.shape["row"], mesh.shape["col"]),
        mesh=mesh,
        in_specs=(
            P(("row", "col"), None),
            P("col", "row", None),
            P("col", "row", None),
            P("row", "col", None),
            P("row"),
            P("col"),
        ),
        out_specs=(P("col", "row", None), P("row", "col", None), P("row", "col", None, None)),
        check_vma=False,
    )
```

```python
import functools

import jax
import jax.numpy as jnp
from jax import lax
from jax.experimental import pallas as pl
from jax.experimental.pallas import tpu as pltpu
from jax.sharding import PartitionSpec as P

RSTEP = 64
BLOCK = 128
SUB = 8
HI = lax.Precision.HIGHEST


def dot_nn(a, b):
    return lax.dot_general(a, b, (((1,), (0,)), ((), ())), precision=HI, preferred_element_type=jnp.float32)


def dot_nt(a, b):
    return lax.dot_general(a, b, (((1,), (1,)), ((), ())), precision=HI, preferred_element_type=jnp.float32)


def factor_block(d_ref, t_ref):
    size = d_ref.shape[0]
    steps = size // SUB
    shape = (SUB, size)
    lane = lax.broadcasted_iota(jnp.int32, shape, 1)
    sub = lax.broadcasted_iota(jnp.int32, shape, 0)
    rows = [d_ref[SUB * i : SUB * (i + 1), :] for i in range(steps)]
    for p in range(steps):
        base = SUB * p
        pivot = (lane >= base) & (lane < base + SUB)
        top = rows[p]
        cols = [jnp.broadcast_to(top[:, base + s : base + s + 1], shape) for s in range(SUB)]
        e = [[jnp.broadcast_to(cols[s][i : i + 1, :], shape) if s <= i else None for s in range(SUB)] for i in range(SUB)]
        top = jnp.where(pivot, jnp.where(lane - base == sub, 1.0, 0.0), top)
        u = [jnp.broadcast_to(top[s : s + 1, :], shape) for s in range(SUB)]
        inv = [None] * SUB
        for s in range(SUB):
            inv[s] = lax.rsqrt(e[s][s])
            u[s] = u[s] * inv[s]
            for i in range(s + 1, SUB):
                e[i][s] = e[i][s] * inv[s]
            for q in range(s + 1, SUB):
                for i in range(q, SUB):
                    e[i][q] = e[i][q] - e[i][s] * e[q][s]
                u[q] = u[q] - e[q][s] * u[s]
        out = u[0]
        for s in range(1, SUB):
            out = jnp.where(sub == s, u[s], out)
        t_ref[base : base + SUB, :] = jnp.where(lane <= base + sub, out, 0.0)
        z = list(u)
        for s in reversed(range(SUB)):
            z[s] = z[s] * inv[s]
            for q in range(s):
                z[q] = z[q] - e[s][q] * z[s]
        for i in range(p + 1, steps):
            m = rows[i]
            acc = jnp.where(pivot, 0.0, m)
            for s in range(SUB):
                acc = acc - jnp.broadcast_to(m[:, base + s : base + s + 1], shape) * z[s]
            rows[i] = acc


def inverse_kernel(a_ref, xh_ref, xl_ref, low, inv, work, block, tri):
    order = a_ref.shape[0]
    count = order // BLOCK

    def store(r, c0, c1, value):
        hi = value.astype(jnp.bfloat16)
        xh_ref[r : r + BLOCK, c0:c1] = hi
        xl_ref[r : r + BLOCK, c0:c1] = (value - hi.astype(jnp.float32)).astype(jnp.bfloat16)

    def step(j, carry):
        for jj in range(count):
            at = BLOCK * jj

            @pl.when(j == jj)
            def _():
                if jj == 0:
                    work[...] = a_ref[:, :BLOCK]
                    block[...] = a_ref[:BLOCK, :BLOCK]
                else:
                    got = a_ref[at:, at : at + BLOCK] - dot_nt(low[at:, :at], low[at : at + BLOCK, :at])
                    work[at:, :] = got
                    block[...] = got[:BLOCK, :]

        factor_block(block, tri)
        for jj in range(count):
            at = BLOCK * jj

            @pl.when(j == jj)
            def _():
                t = tri[...]
                if jj + 1 < count:
                    low[at + BLOCK :, at : at + BLOCK] = dot_nt(work[at + BLOCK :, :], t)
                if jj:
                    x = -dot_nn(t, dot_nn(low[at : at + BLOCK, :at], inv[:at, :at]))
                    inv[at : at + BLOCK, :at] = x
                    store(at, 0, at, x)
                inv[at : at + BLOCK, at : at + BLOCK] = t
                store(at, at, at + BLOCK, t)
                if jj + 1 < count:
                    inv[at : at + BLOCK, at + BLOCK :] = jnp.zeros((BLOCK, order - at - BLOCK), jnp.float32)
                    xh_ref[at : at + BLOCK, at + BLOCK :] = jnp.zeros((BLOCK, order - at - BLOCK), jnp.bfloat16)
                    xl_ref[at : at + BLOCK, at + BLOCK :] = jnp.zeros((BLOCK, order - at - BLOCK), jnp.bfloat16)

        return carry

    lax.fori_loop(0, count, step, 0)


def inverse_of(tile):
    order = tile.shape[0]
    return pl.pallas_call(
        inverse_kernel,
        out_shape=[jax.ShapeDtypeStruct((order, order), jnp.bfloat16)] * 2,
        in_specs=[pl.BlockSpec(memory_space=pltpu.VMEM)],
        out_specs=[pl.BlockSpec(memory_space=pltpu.VMEM)] * 2,
        scratch_shapes=[
            pltpu.VMEM((order, order), jnp.float32),
            pltpu.VMEM((order, order), jnp.float32),
            pltpu.VMEM((order, BLOCK), jnp.float32),
            pltpu.VMEM((BLOCK, BLOCK), jnp.float32),
            pltpu.VMEM((BLOCK, BLOCK), jnp.float32),
        ],
        compiler_params=pltpu.CompilerParams(vmem_limit_bytes=40 * 2**20),
        cost_estimate=pl.CostEstimate(flops=4 * 10**9, bytes_accessed=8 * order * order, transcendentals=0),
    )(tile)


def gather_kernel(rows, cols, groups, x_ref, out_ref, send_sem, recv_sem):
    order = out_ref.shape[2]
    pairs = rows // groups // 2
    row = lax.axis_index("row")
    col = lax.axis_index("col")
    group = row // (2 * pairs)
    pair = (row // 2) % pairs
    core = row % 2
    offsets = [(a, b) for a in range(pairs) for b in range(cols)]

    def device(g, p, c):
        return {"row": (g * pairs + p) * 2 + core, "col": c}

    def block(g, p, c, k):
        return ((g * pairs + p) * 2 + k) * cols + c

    def width(g):
        return -(-order * (g + 1) // (groups * BLOCK)) * BLOCK

    def copy(source, index, wide, sem, target):
        return pltpu.make_async_remote_copy(
            src_ref=source.at[:, :wide],
            dst_ref=out_ref.at[index, :, :wide],
            send_sem=send_sem.at[sem],
            recv_sem=recv_sem.at[index],
            device_id=target,
            device_id_type=pl.DeviceIdType.MESH,
        )

    partner = {"row": (group * pairs + pair) * 2 + 1 - core, "col": col}
    ring = [device((group + k) % groups, pair, col) for k in range(1, groups)]
    plane = [device(group, (pair + a) % pairs, (col + b) % cols) for a, b in offsets[1:]]
    barrier = pltpu.get_barrier_semaphore()
    for peer in ring + plane + [partner]:
        pl.semaphore_signal(barrier, inc=1, device_id=peer, device_id_type=pl.DeviceIdType.MESH)
    pl.semaphore_wait(barrier, len(ring) + len(plane) + 1)

    own = block(group, pair, col, core)
    for g in range(groups):

        @pl.when(group == g)
        def _():
            for k, peer in enumerate(ring):
                copy(x_ref, own, width(g), k, peer).start()
            for k, peer in enumerate(plane):
                copy(x_ref, own, width(g), groups + g * len(offsets) + k, peer).start()
            copy(x_ref, own, width(g), groups * (1 + len(offsets)) + g * len(offsets), partner).start()

    out_ref[own] = x_ref[...]
    for g in range(groups):

        @pl.when(group != g)
        def _():
            index = block(g, pair, col, core)
            got = out_ref.at[index]
            copy(got, index, width(g), 0, partner).wait_recv()
            for k, peer in enumerate(plane):
                copy(got, index, width(g), groups + g * len(offsets) + k, peer).start()
            copy(got, index, width(g), groups * (1 + len(offsets)) + g * len(offsets), partner).start()

    for g in range(groups):
        for n, (a, b) in enumerate(offsets):
            if n:
                index = block(g, (pair + a) % pairs, (col + b) % cols, core)
                got = out_ref.at[index]
                copy(got, index, width(g), 0, partner).wait_recv()
                copy(got, index, width(g), groups * (1 + len(offsets)) + g * len(offsets) + n, partner).start()

    for g in range(groups):
        for n, (a, b) in enumerate(offsets):
            index = block(g, (pair + a) % pairs, (col + b) % cols, 1 - core)
            copy(out_ref.at[index], index, width(g), 0, partner).wait_recv()

    for g in range(groups):

        @pl.when(group == g)
        def _():
            for k, peer in enumerate(ring):
                copy(x_ref, own, width(g), k, peer).wait_send()

        for k, peer in enumerate(plane):
            copy(x_ref, own, width(g), groups + g * len(offsets) + k, peer).wait_send()
        for n in range(len(offsets)):
            copy(x_ref, own, width(g), groups * (1 + len(offsets)) + g * len(offsets) + n, partner).wait_send()


def gather_tile(part, rows, cols):
    high, order = part.shape
    groups = 4 if rows % 8 == 0 else 1
    sends = groups * (1 + 2 * (rows // groups // 2) * cols)
    blocks = pl.pallas_call(
        functools.partial(gather_kernel, rows, cols, groups),
        out_shape=jax.ShapeDtypeStruct((rows * cols, high, order), part.dtype),
        in_specs=[pl.BlockSpec(memory_space=pltpu.VMEM)],
        out_specs=pl.BlockSpec(memory_space=pltpu.VMEM),
        scratch_shapes=[pltpu.SemaphoreType.DMA((sends,)), pltpu.SemaphoreType.DMA((rows * cols,))],
        compiler_params=pltpu.CompilerParams(collective_id=0, has_side_effects=True),
        cost_estimate=pl.CostEstimate(flops=60 * 10**9, bytes_accessed=4 * order * order, transcendentals=0),
    )(part)
    return blocks.reshape(order, order)


def tail_kernel(xh_ref, xl_ref, v_ref, w_ref, u_ref, row_ref, col_ref, out_ref, coupling):
    order = xh_ref.shape[0]
    tiles = out_ref.shape[1]
    rank = v_ref.shape[1]
    chunk = 256

    def solve(src, dst):
        for at in range(0, order, chunk):
            end = at + chunk
            got = jnp.dot(xh_ref[at:end, :end], src[:end, :], preferred_element_type=jnp.float32)
            got = got + jnp.dot(xl_ref[at:end, :end], src[:end, :], preferred_element_type=jnp.float32)
            dst[at:end, :] = got.astype(jnp.bfloat16)

    @pl.when(pl.program_id(0) == 0)
    def _():
        for j in range(tiles):
            solve(w_ref.at[:, rank * j : rank * (j + 1)], col_ref.at[:, rank * j : rank * (j + 1)])

    solve(v_ref, row_ref)
    coupling[...] = lax.dot_general(
        row_ref[...], col_ref[...], (((0,), (0,)), ((), ())), preferred_element_type=jnp.float32
    ).astype(jnp.bfloat16)
    for j in range(tiles):
        for at in range(0, order, chunk):
            got = jnp.dot(
                u_ref[at : at + chunk, :], coupling[:, rank * j : rank * (j + 1)], preferred_element_type=jnp.float32
            )
            out_ref[0, j, at : at + chunk, :] = (-got).astype(jnp.bfloat16)


def tail(high, low, v, w, u, rank):
    order = high.shape[0]
    count, tiles = v.shape[1] // rank, w.shape[1] // rank
    whole = pl.BlockSpec((order, order), lambda i: (0, 0))
    wide = pl.BlockSpec(w.shape, lambda i: (0, 0))
    one = pl.BlockSpec((order, rank), lambda i: (0, i))
    return pl.pallas_call(
        tail_kernel,
        grid=(count,),
        out_shape=[
            jax.ShapeDtypeStruct(v.shape, jnp.bfloat16),
            jax.ShapeDtypeStruct(w.shape, jnp.bfloat16),
            jax.ShapeDtypeStruct((count, tiles, order, rank), jnp.bfloat16),
        ],
        in_specs=[whole, whole, one, wide, one],
        out_specs=[one, wide, pl.BlockSpec((1, tiles, order, rank), lambda i: (i, 0, 0, 0))],
        scratch_shapes=[pltpu.VMEM((rank, w.shape[1]), jnp.bfloat16)],
        compiler_params=pltpu.CompilerParams(vmem_limit_bytes=50 * 2**20),
        cost_estimate=pl.CostEstimate(flops=8 * 10**9, bytes_accessed=18 * order * order, transcendentals=0),
    )(high, low, v, w, u)


def mask_columns(right, bucket):
    live = jnp.arange(right.shape[2], dtype=jnp.int32)[None, :] < (RSTEP * bucket)[:, None]
    return jnp.where(live[None, :, :], right, jnp.zeros_like(right))


def per_device(rows, cols, diag_tile, left_row, right_row, right_col, bucket_row, bucket_col):
    rank = right_row.shape[2]
    flat_col = mask_columns(right_col, bucket_col).reshape(right_col.shape[0], -1)
    flat_col, diag_tile = lax.optimization_barrier((flat_col, diag_tile))
    w = lax.all_gather(flat_col, "row", axis=0, tiled=True)
    whole_tile = gather_tile(diag_tile, rows, cols)
    whole_tile, right_row, left_row = lax.optimization_barrier((whole_tile, right_row, left_row))
    flat_row = mask_columns(right_row, bucket_row).reshape(right_row.shape[0], -1)
    flat_left = left_row.reshape(left_row.shape[0], -1)
    v = lax.all_gather(flat_row, "col", axis=0, tiled=True)
    u = lax.all_gather(flat_left, "col", axis=0, tiled=True)
    high, low = inverse_of(whole_tile)
    full_row, full_col, update_left = tail(high, low, v, w, u, rank)
    panel_row = lax.dynamic_slice_in_dim(
        full_row, lax.axis_index("col") * flat_row.shape[0], flat_row.shape[0], 0
    ).reshape(right_row.shape)
    panel_col = lax.dynamic_slice_in_dim(
        full_col, lax.axis_index("row") * flat_col.shape[0], flat_col.shape[0], 0
    ).reshape(right_col.shape)
    return (panel_row, panel_col, update_left)


def solution(mesh):
    return jax.shard_map(
        functools.partial(per_device, mesh.shape["row"], mesh.shape["col"]),
        mesh=mesh,
        in_specs=(
            P(("row", "col"), None),
            P("col", "row", None),
            P("col", "row", None),
            P("row", "col", None),
            P("row"),
            P("col"),
        ),
        out_specs=(P("col", "row", None), P("row", "col", None), P("row", "col", None, None)),
        check_vma=False,
    )
```
